32 devices in a mesh: ep: 4 (over z), fsdp: 8 (over y, x, core).
Axes of the slice: x: 2, y: 2, z: 4, core: 2. Of those that a mesh axis runs over, the one named last changes fastest.
Arguments:
- train_gate: float32 [64, 2048, 1408], P('ep', 'fsdp'), may hold values from -0.1875 to 0.1875
- train_up: float32 [64, 2048, 1408], P('ep', 'fsdp'), may hold values from -0.1875 to 0.1875
- train_down: float32 [64, 1408, 2048], P('ep', None, 'fsdp'), may hold values from -0.21875 to 0.21875
- router_weight: float32 [2048, 64], P('fsdp', 'ep'), may hold values from -0.125 to 0.125
- router_gain: float32 [2048], P('fsdp'), may hold values from 0.25 to 1.75
Outputs:
- ready_gate: bfloat16 [64, 2048, 1408], P('ep', None, 'fsdp')
- ready_up: bfloat16 [64, 2048, 1408], P('ep', None, 'fsdp')
- ready_down: bfloat16 [64, 1408, 2048], P('ep', 'fsdp')
- scale_gate: float32 [64, 1408], P('ep', 'fsdp')
- scale_up: float32 [64, 1408], P('ep', 'fsdp')
- scale_down: float32 [64, 1408], P('ep', 'fsdp')
- serve_router: bfloat16 [2048, 64], replicated
The draws below stay inside these ranges and needn't reach their ends.
All inputs are finite; a program needn't handle non-finite values.
Results may differ from the reference program's by a relative error of at most 0.001.
Values may be sent and summed in bfloat16 or wider, within the bound.
A program may use at most 192 MiB of HBM per device.

```python
import jax
import jax.numpy as jnp
from jax import lax

EXPERTS = 64
D_MODEL = 2048
D_EXPERT = 1408


def strengthened(drawn, own_key, source, target, shards_of, factor):
    owner, partner = [(jnp.arange(drawn.shape[axis_at]) // (drawn.shape[axis_at] // shards_of)).reshape([-1 if axis == axis_at else 1 for axis in range(drawn.ndim)]) for axis_at in (source, target)]
    chosen = jax.random.permutation(own_key, shards_of)[partner]
    strong = (owner == chosen) | (owner == (partner + shards_of // 2) % shards_of)
    return jnp.where(strong, factor * drawn, drawn)


def block_scale(rng, extent, cuts, smallest, largest):
    gain, own = 1.0, jax.random.fold_in(rng, 6)
    for axis_at, blocks in cuts:
        steps = jnp.exp(jax.random.uniform(jax.random.fold_in(own, axis_at), (blocks,), jnp.float32, smallest / len(cuts), largest / len(cuts)))
        gain = gain * jnp.repeat(steps, extent[axis_at] // blocks).reshape([-1 if axis == axis_at else 1 for axis in range(len(extent))])
    return gain


def normal_values(rng, extent, width, reach, pieces=(), dtype=jnp.bfloat16):
    loudness = block_scale(rng, extent, pieces, -0.22, 0.18) if pieces else 1.0
    result = jax.random.normal(rng, extent, jnp.float32) * width * loudness
    return jnp.minimum(jnp.maximum(result, -reach), reach).astype(dtype)


def bell_draw_with(own_key, dims, width, reach, shards, heavy, held_as=jnp.bfloat16):
    values = width * jax.random.normal(own_key, dims, jnp.float32)
    if shards:
        values = values * block_scale(own_key, dims, shards, -0.22, 0.18)
    return jnp.clip(strengthened(values, jax.random.fold_in(own_key, 3), *heavy), -reach, reach).astype(held_as)


def setup_inputs(seed: int = 0) -> dict:
    seeds = jax.random.split(jax.random.key(seed), 6)
    return {
        "train_gate": bell_draw_with(seeds[0], (EXPERTS, D_MODEL, D_EXPERT), D_MODEL ** -0.5, 0.1875, ((0, 4), (1, 8)), (1, 2, 8, 2.0), jnp.float32),
        "train_up": bell_draw_with(seeds[1], (EXPERTS, D_MODEL, D_EXPERT), D_MODEL ** -0.5, 0.1875, ((0, 4), (1, 8)), (1, 2, 8, 2.0), jnp.float32),
        "train_down": bell_draw_with(seeds[2], (EXPERTS, D_EXPERT, D_MODEL), D_EXPERT ** -0.5, 0.21875, ((0, 4), (2, 8)), (2, 1, 8, 2.0), jnp.float32),
        "router_weight": normal_values(seeds[3], (D_MODEL, EXPERTS), D_MODEL ** -0.5, 0.125, ((0, 8), (1, 4)), jnp.float32),
        "router_gain": jnp.clip(1.0 + 0.15 * jax.random.normal(seeds[4], (D_MODEL,), jnp.float32), 0.25, 1.75),
    }


def reference(train_gate, train_up, train_down, router_weight, router_gain):
    scale_gate = jnp.sqrt(lax.optimization_barrier(jnp.sum(train_gate * train_gate, axis=1)))
    ready_gate = (train_gate / jnp.expand_dims(scale_gate, 1)).astype(jnp.bfloat16)
    scale_up = jnp.sqrt(lax.optimization_barrier(jnp.sum(train_up * train_up, axis=1)))
    ready_up = (train_up / jnp.expand_dims(scale_up, 1)).astype(jnp.bfloat16)
    scale_down = jnp.sqrt(lax.optimization_barrier(jnp.sum(train_down * train_down, axis=2)))
    ready_down = (train_down / jnp.expand_dims(scale_down, 2)).astype(jnp.bfloat16)
    serve_router = (router_weight * router_gain[:, None]).astype(jnp.bfloat16)
    return (ready_gate, ready_up, ready_down, scale_gate, scale_up, scale_down, serve_router)
```

```python
import functools

import jax
import jax.numpy as jnp
from jax import lax
from jax.experimental import pallas as pl
from jax.experimental.pallas import tpu as pltpu
from jax.sharding import PartitionSpec as P

MESH = pl.DeviceIdType.MESH
VMEM = pltpu.VMEM
PAIR = 2
SLOTS = 2
KINDS = 3
LATE = (1, 2)


def bits_of(n):
    return n.bit_length() - 1


def plain_body(train_gate, train_up, train_down, router_weight, router_gain):
    total_gate, total_up, total_down = lax.psum(
        (
            jnp.sum(train_gate * train_gate, axis=1),
            jnp.sum(train_up * train_up, axis=1),
            jnp.sum(train_down * train_down, axis=2),
        ),
        "fsdp",
    )
    scale_gate = jnp.sqrt(total_gate)
    scale_up = jnp.sqrt(total_up)
    scale_down = jnp.sqrt(total_down)
    narrow_gate, narrow_up, narrow_down = (
        (train_gate / jnp.expand_dims(scale_gate, 1)).astype(jnp.bfloat16),
        (train_up / jnp.expand_dims(scale_up, 1)).astype(jnp.bfloat16),
        (train_down / jnp.expand_dims(scale_down, 2)).astype(jnp.bfloat16),
    )
    ready_gate = lax.all_to_all(narrow_gate, "fsdp", split_axis=2, concat_axis=1, tiled=True)
    ready_up = lax.all_to_all(narrow_up, "fsdp", split_axis=2, concat_axis=1, tiled=True)
    ready_down = lax.all_to_all(narrow_down, "fsdp", split_axis=1, concat_axis=2, tiled=True)
    piece = ready_gate.shape[2]
    mine = lambda s: lax.dynamic_slice_in_dim(s, lax.axis_index("fsdp") * piece, piece, axis=1)
    part_router = (router_weight * router_gain[:, None]).astype(jnp.bfloat16)
    row_router = lax.all_gather(part_router, "fsdp", axis=0, tiled=True)
    serve_router = lax.all_gather(row_router, "ep", axis=1, tiled=True)
    return (ready_gate, ready_up, ready_down, mine(scale_gate), mine(scale_up), mine(scale_down), serve_router)


def column_of(row, width):
    return jnp.broadcast_to(row, (width, row.shape[1])).T


def flip(i, w):
    return i + w - 2 * w * ((i // w) % 2)


def other(i, k):
    for b in range(bits_of(k) + 1):
        if (k >> b) & 1:
            i = flip(i, 1 << b)
    return i


def square_sums(turned, x):
    x = x * x
    if turned:
        return jnp.sum(x, axis=0, keepdims=True)
    folded = x[:, :128]
    for at in range(128, x.shape[1], 128):
        folded = folded + x[:, at : at + 128]
    return jnp.sum(folded.T, axis=0, keepdims=True)


def route_kernel(n_ep, n, pairs, *refs):
    fb = bits_of(n)
    sources, (weight_ref, gain_ref), refs = refs[:KINDS], refs[KINDS : KINDS + 2], refs[KINDS + 2 :]
    lands, (scale_ref, all_ref), refs = refs[:KINDS], refs[KINDS : KINDS + 2], refs[KINDS + 2 :]
    late_refs, refs = refs[:n], refs[n:]
    held, refs = refs[:KINDS], refs[KINDS:]
    packed, part, total, landed, lsem, ssend, srecv, bsend, brecv, osem, rsend, rrecv = refs
    ep, me = lax.axis_index("ep"), lax.axis_index("fsdp")
    core = me % 2
    piece = packed.shape[3]
    last = pairs - 1

    ep_peers = [((ep + d) % n_ep, me) for d in range(1, n_ep)]
    fsdp_peers = [(ep, other(me, k)) for k in range(1, n)]
    sum_peers = [(ep, flip(me, 1))] + [
        (ep, flip(me, (1 << k) * (1 - core) + (1 << (fb - k)) * core)) for k in range(1, fb)
    ]

    def load(t, p):
        return pltpu.make_async_copy(
            sources[t].at[pl.ds(p * PAIR, PAIR)], held[t].at[p % SLOTS], lsem.at[t, p % SLOTS]
        )

    for p in range(SLOTS):
        for t in range(KINDS):
            load(t, p).start()

    barrier = pltpu.get_barrier_semaphore()
    for peer in ep_peers + fsdp_peers:
        pl.semaphore_signal(barrier, inc=1, device_id=peer, device_id_type=MESH)
    all_ref[ep, me // 2, core] = (weight_ref[...] * gain_ref[...]).astype(all_ref.dtype)
    pl.semaphore_wait(barrier, n_ep - 1 + n - 1)

    def sum_copy(k, t, p):
        s = p % SLOTS
        if k == 0:
            src, dst, peer = part.at[t, s, 1 - core], landed.at[t, s, 0], sum_peers[0]
        elif k < fb:
            src, dst, peer = total.at[t, s, k - 1], landed.at[t, s, k], sum_peers[k]
        else:
            src = dst = scale_ref.at[t, p * PAIR + core]
            peer = sum_peers[0]
        return pltpu.make_async_remote_copy(
            src, dst, ssend.at[t, s, k], srecv.at[t, s, k], device_id=peer, device_id_type=MESH
        )

    def begin_sums(t, p):
        s = p % SLOTS
        load(t, p).wait()
        for i in range(PAIR):
            part[t, s, i] = square_sums(t < 2, held[t][s, i])
        sum_copy(0, t, p).start()

    def step_sums(k, t, p):
        s = p % SLOTS
        sum_copy(k, t, p).wait()
        value = (part[t, s, core] if k == 0 else total[t, s, k - 1]) + landed[t, s, k]
        if k < fb - 1:
            total[t, s, k] = value
        else:
            scale_ref[t, p * PAIR + core] = jnp.sqrt(value)
        sum_copy(k + 1, t, p).start()

    def bulk_copies(t, p):
        dst = lands[t].at[me, pl.ds(p * PAIR, PAIR)]
        copies = [pltpu.make_async_copy(packed.at[t, me], dst, bsend.at[t, 0])]
        for k in [6, 7, 2, 4, 3, 5, 1] if n == 8 else range(1, n):
            copies.append(
                pltpu.make_async_remote_copy(
                    packed.at[t, other(me, k)],
                    dst,
                    bsend.at[t, k],
                    brecv.at[t, k],
                    device_id=(ep, other(me, k)),
                    device_id_type=MESH,
                )
            )
        return copies

    def finish_bulk(t, p):
        copies = bulk_copies(t, p)
        copies[0].wait()
        for c in copies[1:]:
            c.wait_send()

    def late_copies(t):
        at = LATE.index(t)
        return [
            pltpu.make_async_copy(packed.at[t, other(me, k)], late_refs[k].at[at], osem.at[at, k]) for k in range(n)
        ]

    def send(t, p):
        s = p % SLOTS
        sum_copy(fb, t, p).wait()

        @pl.when(p > 0)
        def _():
            finish_bulk(t, p - 1)

        for i in range(PAIR):
            inverse = 1.0 / scale_ref[t, p * PAIR + i]
            if t < 2:
                y = (held[t][s, i] * inverse).astype(packed.dtype).T
                for j in range(n):
                    packed[t, j, i] = y[j * piece : (j + 1) * piece, :]
            else:
                column = column_of(inverse, 128)
                for at in range(0, held[t].shape[3], 128):
                    y = (held[t][s, i, :, at : at + 128] * column).astype(packed.dtype)
                    for j in range(n):
                        packed[t, j, i, :, at : at + 128] = y[j * piece : (j + 1) * piece, :]
        if t in LATE:

            @pl.when(p < last)
            def _():
                for c in bulk_copies(t, p):
                    c.start()

            @pl.when(p == last)
            def _():
                for c in late_copies(t):
                    c.start()

        else:
            for c in bulk_copies(t, p):
                c.start()

        @pl.when(p + SLOTS < pairs)
        def _():
            load(t, p + SLOTS).start()

    def router_copies(k):
        if k == 0:
            block = all_ref.at[ep, me // 2, core]
            jobs = [(d, peer) for d, peer in enumerate(ep_peers)]
        elif k == 1:
            block = all_ref.at[:, me // 2, core]
            jobs = [(n_ep - 2 + c, fsdp_peers[2 * c - 1]) for c in range(1, n // 2)]
        else:
            block = all_ref.at[:, :, core]
            jobs = [(n_ep - 2 + n // 2, sum_peers[0])]
        return [
            pltpu.make_async_remote_copy(block, block, rsend.at[i], rrecv.at[i], device_id=peer, device_id_type=MESH)
            for i, peer in jobs
        ]

    for c in router_copies(0):
        c.start()

    lag = fb + 1
    for u in range(-lag, 0):
        for k in range(fb, 0, -1):
            v = u + lag - k
            if v >= 0:
                step_sums(k - 1, v % KINDS, v // KINDS)
        begin_sums((u + lag) % KINDS, (u + lag) // KINDS)

    def later(t, p, ahead, act):
        at, q = (t + ahead) % KINDS, p + (t + ahead) // KINDS

        @pl.when(q < pairs)
        def _():
            act(at, q)

    def loop(p, carry):
        for t in range(KINDS):
            send(t, p)
            for k in range(fb, 0, -1):
                later(t, p, lag - k, functools.partial(step_sums, k - 1))
            later(t, p, lag, begin_sums)
        for k in (1, 2):

            @pl.when(p == 2 * k - 1)
            def _():
                for c in router_copies(k - 1):
                    c.wait()
                for c in router_copies(k):
                    c.start()

        return carry

    lax.fori_loop(0, pairs, loop, 0)

    for c in router_copies(2):
        c.wait()
    for t in range(KINDS):
        if t in LATE:
            for c in late_copies(t):
                c.wait()
        else:
            finish_bulk(t, last)
        for k in range(1, n):
            arrived = lands[t].at[other(me, k)]
            pltpu.make_async_copy(arrived, arrived, brecv.at[t, k]).wait()


def route(mesh, gate, up, down, weight, gain):
    n_ep, n = mesh.shape["ep"], mesh.shape["fsdp"]
    experts, rows, wide = gate.shape
    piece, fb, pairs = wide // n, bits_of(n), experts // PAIR
    vmem, hbm = pl.BlockSpec(memory_space=VMEM), pl.BlockSpec(memory_space=pl.ANY)
    dma = pltpu.SemaphoreType.DMA
    half = jnp.bfloat16
    land = lambda t: jax.ShapeDtypeStruct((n, experts - PAIR * (t in LATE), piece, rows), half)
    outs = pl.pallas_call(
        functools.partial(route_kernel, n_ep, n, pairs),
        out_shape=tuple(land(t) for t in range(KINDS))
        + (
            jax.ShapeDtypeStruct((KINDS, experts, 1, wide), jnp.float32),
            jax.ShapeDtypeStruct((n_ep, n // 2, 2) + weight.shape, half),
        )
        + tuple(jax.ShapeDtypeStruct((len(LATE), PAIR, piece, rows), half) for _ in range(n)),
        in_specs=[hbm] * KINDS + [vmem] * 2,
        out_specs=tuple([hbm] * KINDS + [vmem] * 2 + [hbm] * n),
        scratch_shapes=[
            VMEM((SLOTS, PAIR, rows, wide), jnp.float32),
            VMEM((SLOTS, PAIR, rows, wide), jnp.float32),
            VMEM((SLOTS, PAIR, wide, rows), jnp.float32),
            VMEM((KINDS, n, PAIR, piece, rows), half),
            VMEM((KINDS, SLOTS, PAIR, 1, wide), jnp.float32),
            VMEM((KINDS, SLOTS, fb - 1, 1, wide), jnp.float32),
            VMEM((KINDS, SLOTS, fb, 1, wide), jnp.float32),
            dma((KINDS, SLOTS)),
            dma((KINDS, SLOTS, fb + 1)),
            dma((KINDS, SLOTS, fb + 1)),
            dma((KINDS, n)),
            dma((KINDS, n)),
            dma((len(LATE), n)),
            dma((n_ep - 1 + n // 2,)),
            dma((n_ep - 1 + n // 2,)),
        ],
        compiler_params=pltpu.CompilerParams(collective_id=0, has_side_effects=True),
        cost_estimate=pl.CostEstimate(flops=12 * gate.size, bytes_accessed=18 * gate.size, transcendentals=0),
        name="route",
    )(gate, up, down, weight, gain)
    return outs[:KINDS], outs[KINDS], outs[KINDS + 1], outs[KINDS + 2 :]


def place_kernel(in_ref, out_ref):
    pieces, block, _, rows = in_ref.shape
    for i in range(block):
        for s in range(pieces):
            out_ref[i, :, s * rows : (s + 1) * rows] = in_ref[s, i]


def place(x, experts, name, block=PAIR):
    pieces, landed, piece, rows = x.shape
    shape = (piece, pieces * rows)
    return pl.pallas_call(
        place_kernel,
        grid=(landed // block,),
        out_shape=jax.ShapeDtypeStruct((experts,) + shape, x.dtype),
        in_specs=[pl.BlockSpec((pieces, block, piece, rows), lambda e: (0, e, 0, 0))],
        out_specs=pl.BlockSpec((block,) + shape, lambda e: (e, 0, 0)),
        cost_estimate=pl.CostEstimate(flops=x.size, bytes_accessed=4 * x.size, transcendentals=0),
        name=name,
    )(x)


def finish_kernel(n, count, *refs):
    got, outs = refs[:n], refs[n + count :]
    me = lax.axis_index("fsdp")
    rows = got[0].shape[3]
    for k in range(n):
        at = pl.multiple_of(other(me, k) * rows, 128)
        for t in range(count):
            outs[t][0, :, pl.ds(at, rows)] = got[k][t, 0]


def finish(got, arrays):
    n, count = len(got), len(arrays)
    _, _, piece, rows = got[0].shape
    experts = arrays[0].shape[0]
    return pl.pallas_call(
        functools.partial(finish_kernel, n, count),
        grid=(PAIR,),
        out_shape=tuple(jax.ShapeDtypeStruct(a.shape, a.dtype) for a in arrays),
        in_specs=[pl.BlockSpec((count, 1, piece, rows), lambda e: (0, e, 0, 0))] * n
        + [pl.BlockSpec(memory_space=pl.ANY)] * count,
        out_specs=tuple([pl.BlockSpec((1, piece, n * rows), lambda e: (experts - PAIR + e, 0, 0))] * count),
        input_output_aliases={n + t: t for t in range(count)},
        cost_estimate=pl.CostEstimate(flops=n * got[0].size, bytes_accessed=4 * n * got[0].size, transcendentals=0),
        name="finish",
    )(*got, *arrays)


def body(mesh, train_gate, train_up, train_down, router_weight, router_gain):
    n = mesh.shape["fsdp"]
    experts, rows, wide = train_gate.shape
    piece = wide // n
    lands, scale, gathered, late = route(
        mesh, train_gate, train_up, train_down, router_weight.T, router_gain[None, :]
    )
    got = (late[0],) + tuple(
        lax.ppermute(late[k], "fsdp", [(i, i ^ k) for i in range(n)]) for k in range(1, n)
    )
    placed = [place(x, experts, name) for x, name in zip(lands, ("place_gate", "place_up", "place_down"))]
    done = finish(got, tuple(placed[t] for t in LATE))
    for t, array in zip(LATE, done):
        placed[t] = array
    ready_gate, ready_up, ready_down = placed[0].swapaxes(1, 2), placed[1].swapaxes(1, 2), placed[2]

    mine = lax.dynamic_slice_in_dim(scale[:, :, 0], lax.axis_index("fsdp") * piece, piece, axis=2)
    serve_router = gathered.transpose(0, 3, 1, 2, 4).reshape(-1, n * rows).T
    return (ready_gate, ready_up, ready_down, mine[0], mine[1], mine[2], serve_router)


def solution(mesh):
    def step(gate, up, down, weight, gain):
        n_ep, n = mesh.shape["ep"], mesh.shape["fsdp"]
        experts, rows, wide = gate.shape
        fits = n & (n - 1) == 0 and n_ep > 1 and 2 < n and bits_of(n) + 1 < SLOTS * KINDS
        if fits and rows % 128 == 0 and wide % (16 * n) == 0 and wide % 128 == 0 and experts % PAIR == 0 and experts >= 8 * PAIR:
            return body(mesh, gate, up, down, weight, gain)
        return plain_body(gate, up, down, weight, gain)

    return jax.shard_map(
        step,
        mesh=mesh,
        in_specs=(
            P("ep", "fsdp", None),
            P("ep", "fsdp", None),
            P("ep", None, "fsdp"),
            P("fsdp", "ep"),
            P("fsdp"),
        ),
        out_specs=(
            P("ep", None, "fsdp"),
            P("ep", None, "fsdp"),
            P("ep", "fsdp", None),
            P("ep", "fsdp"),
            P("ep", "fsdp"),
            P("ep", "fsdp"),
            P(),
        ),
        check_vma=False,
    )
```

```python
import functools

import jax
import jax.numpy as jnp
from jax import lax
from jax.experimental import pallas as pl
from jax.experimental.pallas import tpu as pltpu
from jax.sharding import PartitionSpec as P

MESH = pl.DeviceIdType.MESH
VMEM = pltpu.VMEM
PAIR = 2
SLOTS = 3
KINDS = 3
LATE = (1, 2)
AHEAD = (6, 5, 3, 1)


def bits_of(n):
    return n.bit_length() - 1


def plain_body(train_gate, train_up, train_down, router_weight, router_gain):
    total_gate, total_up, total_down = lax.psum(
        (
            jnp.sum(train_gate * train_gate, axis=1),
            jnp.sum(train_up * train_up, axis=1),
            jnp.sum(train_down * train_down, axis=2),
        ),
        "fsdp",
    )
    scale_gate = jnp.sqrt(total_gate)
    scale_up = jnp.sqrt(total_up)
    scale_down = jnp.sqrt(total_down)
    narrow_gate, narrow_up, narrow_down = (
        (train_gate / jnp.expand_dims(scale_gate, 1)).astype(jnp.bfloat16),
        (train_up / jnp.expand_dims(scale_up, 1)).astype(jnp.bfloat16),
        (train_down / jnp.expand_dims(scale_down, 2)).astype(jnp.bfloat16),
    )
    ready_gate = lax.all_to_all(narrow_gate, "fsdp", split_axis=2, concat_axis=1, tiled=True)
    ready_up = lax.all_to_all(narrow_up, "fsdp", split_axis=2, concat_axis=1, tiled=True)
    ready_down = lax.all_to_all(narrow_down, "fsdp", split_axis=1, concat_axis=2, tiled=True)
    piece = ready_gate.shape[2]
    mine = lambda s: lax.dynamic_slice_in_dim(s, lax.axis_index("fsdp") * piece, piece, axis=1)
    part_router = (router_weight * router_gain[:, None]).astype(jnp.bfloat16)
    row_router = lax.all_gather(part_router, "fsdp", axis=0, tiled=True)
    serve_router = lax.all_gather(row_router, "ep", axis=1, tiled=True)
    return (ready_gate, ready_up, ready_down, mine(scale_gate), mine(scale_up), mine(scale_down), serve_router)


def column_of(row, width):
    return jnp.broadcast_to(row, (width, row.shape[1])).T


def flip(i, w):
    return i + w - 2 * w * ((i // w) % 2)


def other(i, k):
    for b in range(bits_of(k) + 1):
        if (k >> b) & 1:
            i = flip(i, 1 << b)
    return i


def square_sums(turned, x):
    x = x * x
    if turned:
        return jnp.sum(x, axis=0, keepdims=True)
    folded = x[:, :128]
    for at in range(128, x.shape[1], 128):
        folded = folded + x[:, at : at + 128]
    return jnp.sum(folded.T, axis=0, keepdims=True)


def route_kernel(n_ep, n, pairs, *refs):
    fb = bits_of(n)
    sources, (weight_src, gain_src), refs = refs[:KINDS], refs[KINDS : KINDS + 2], refs[KINDS + 2 :]
    lands, (scale_out, all_out), refs = refs[:KINDS], refs[KINDS : KINDS + 2], refs[KINDS + 2 :]
    late_refs, refs = refs[:n], refs[n:]
    held, refs = refs[:KINDS], refs[KINDS:]
    weight_ref, gain_ref, scale_ref, all_ref, packed, part, total, landed, first = refs[:9]
    lsem, ssend, srecv, fsend, frecv, bsend, brecv, osem, rsend, rrecv, wsem = refs[9:]
    ep, me = lax.axis_index("ep"), lax.axis_index("fsdp")
    core = me % 2
    piece = packed.shape[3]
    last = pairs - 1

    ep_peers = [((ep + d) % n_ep, me) for d in range(1, n_ep)]
    fsdp_peers = [(ep, other(me, k)) for k in range(1, n)]
    sum_peers = [(ep, flip(me, 1))] + [
        (ep, flip(me, (1 << k) * (1 - core) + (1 << (fb - k)) * core)) for k in range(1, fb)
    ]

    def load(t, p):
        return pltpu.make_async_copy(
            sources[t].at[pl.ds(p * PAIR, PAIR)], held[t].at[p % SLOTS], lsem.at[t, p % SLOTS]
        )

    opening = [(0, i, 1) for i in range(PAIR)] + [(t, 0, PAIR) for t in range(1, KINDS)]

    def first_load(at):
        t, i, count = opening[at]
        return pltpu.make_async_copy(
            sources[t].at[pl.ds(i, count)], held[t].at[0, pl.ds(i, count)], lsem.at[KINDS + at // SLOTS, at % SLOTS]
        )

    def first_copies(at):
        t, i, count = opening[at]
        return [
            pltpu.make_async_remote_copy(
                part.at[t, 0, pl.ds(i, count)],
                first.at[t, me, pl.ds(i, count)],
                fsend.at[at, k - 1],
                frecv.at[at, k - 1],
                device_id=fsdp_peers[k - 1],
                device_id_type=MESH,
            )
            for k in range(1, n)
        ]

    def first_scales(at):
        t, i, count = opening[at]
        for c in first_copies(at):
            c.wait()
        rows = pl.ds(i, count)
        first[t, me, rows] = part[t, 0, rows]
        value = first[t, 0, rows]
        for j in range(1, n):
            value = value + first[t, j, rows]
        scale_ref[t, rows] = jnp.sqrt(value)

    weight_loads = [
        pltpu.make_async_copy(weight_src, weight_ref, wsem.at[0]),
        pltpu.make_async_copy(gain_src, gain_ref, wsem.at[1]),
    ]
    first_load(0).start()
    for c in weight_loads:
        c.start()
    first_load(1).start()
    barrier = pltpu.get_barrier_semaphore()
    for peer in ep_peers + fsdp_peers:
        pl.semaphore_signal(barrier, inc=1, device_id=peer, device_id_type=MESH)

    def sum_copy(k, t, p):
        s = p % SLOTS
        if k == 0:
            src, dst, peer = part.at[t, s, 1 - core], landed.at[t, s, 0], sum_peers[0]
        elif k < fb:
            src, dst, peer = total.at[t, s, k - 1], landed.at[t, s, k], sum_peers[k]
        else:
            src = dst = scale_ref.at[t, p * PAIR + core]
            peer = sum_peers[0]
        return pltpu.make_async_remote_copy(
            src, dst, ssend.at[t, s, k], srecv.at[t, s, k], device_id=peer, device_id_type=MESH
        )

    def begin_sums(t, p):
        s = p % SLOTS
        load(t, p).wait()
        for i in range(PAIR):
            part[t, s, i] = square_sums(t < 2, held[t][s, i])
        sum_copy(0, t, p).start()

    def step_sums(k, t, p):
        s = p % SLOTS
        sum_copy(k, t, p).wait()
        value = (part[t, s, core] if k == 0 else total[t, s, k - 1]) + landed[t, s, k]
        if k < fb - 1:
            total[t, s, k] = value
        else:
            scale_ref[t, p * PAIR + core] = jnp.sqrt(value)
        sum_copy(k + 1, t, p).start()

    nearest = sorted(range(1, n), key=lambda k: (k < 2, bin(k // 2).count("1"), k % 2, -k))

    def bulk_copies(t, p, i, count):
        dst = lands[t].at[me, pl.ds(p * PAIR + i, count)]
        copies = [
            pltpu.make_async_remote_copy(
                packed.at[t, other(me, k), pl.ds(i, count)],
                dst,
                bsend.at[t, k],
                brecv.at[t, k],
                device_id=(ep, other(me, k)),
                device_id_type=MESH,
            )
            for k in nearest
        ]
        return copies, pltpu.make_async_copy(packed.at[t, me, pl.ds(i, count)], dst, bsend.at[t, 0])

    def start_bulk(t, p, i, count):
        remote, local = bulk_copies(t, p, i, count)
        for c in remote:
            c.start()
        local.start()

    def finish_bulk(t, p):
        remote, local = bulk_copies(t, p, 0, PAIR)
        for c in remote:
            c.wait_send()
        local.wait()

    def late_copies(t):
        at = LATE.index(t)
        return [
            pltpu.make_async_copy(packed.at[t, other(me, k)], late_refs[k].at[at], osem.at[at, k]) for k in range(n)
        ]

    def send(t, p):
        s = p % SLOTS

        @pl.when(p > 0)
        def _():
            sum_copy(fb, t, p).wait()
            finish_bulk(t, p - 1)

        for i in range(PAIR):

            @pl.when(p == 0)
            def _():
                if (t, i, 1) in opening:
                    first_scales(opening.index((t, i, 1)))
                elif i == 0:
                    first_scales(opening.index((t, i, PAIR)))

            inverse = 1.0 / scale_ref[t, p * PAIR + i]
            if t < 2:
                y = (held[t][s, i] * inverse).astype(packed.dtype).T
                for j in range(n):
                    packed[t, j, i] = y[j * piece : (j + 1) * piece, :]
            else:
                column = column_of(inverse, 128)
                for at in range(0, held[t].shape[3], 128):
                    y = (held[t][s, i, :, at : at + 128] * column).astype(packed.dtype)
                    for j in range(n):
                        packed[t, j, i, :, at : at + 128] = y[j * piece : (j + 1) * piece, :]
            if (t, i, 1) in opening:

                @pl.when(p == 0)
                def _():
                    start_bulk(t, p, i, 1)

        split = (t, 0, 1) in opening

        @pl.when((p >= split) & (p < last + (t not in LATE)))
        def _():
            start_bulk(t, p, 0, PAIR)

        if t in LATE:

            @pl.when(p == last)
            def _():
                for c in late_copies(t):
                    c.start()

        @pl.when(p + SLOTS < pairs)
        def _():
            load(t, p + SLOTS).start()

    def router_copies(k):
        if k == 0:
            block = all_ref.at[ep, me // 2, core]
            jobs = [(d, peer) for d, peer in enumerate(ep_peers)]
        elif k == 1:
            block = all_ref.at[:, me // 2, core]
            jobs = [(n_ep - 2 + c, fsdp_peers[2 * c - 1]) for c in range(1, n // 2)]
        else:
            block = all_ref.at[:, :, core]
            jobs = [(n_ep - 2 + n // 2, sum_peers[0])]
        return [
            pltpu.make_async_remote_copy(block, block, rsend.at[i], rrecv.at[i], device_id=peer, device_id_type=MESH)
            for i, peer in jobs
        ]

    for at, (t, i, count) in enumerate(opening):
        first_load(at).wait()
        if at + 2 < len(opening):
            first_load(at + 2).start()
        for e in range(i, i + count):
            part[t, 0, e] = square_sums(t < 2, held[t][0, e])
        if at == 0:
            pl.semaphore_wait(barrier, n_ep - 1 + n - 1)
        for c in first_copies(at):
            c.start()
        if at == 0:
            for c in weight_loads:
                c.wait()
            all_ref[ep, me // 2, core] = (weight_ref[...] * gain_ref[...]).astype(all_ref.dtype)
            for c in router_copies(0):
                c.start()
    for c in router_copies(0):
        c.wait()
    for c in router_copies(1):
        c.start()

    for p in range(1, SLOTS):
        for t in range(KINDS):
            load(t, p).start()

    acts = [begin_sums] + [functools.partial(step_sums, k) for k in range(fb)]

    def later(t, p, j):
        at, q = (t + AHEAD[j]) % KINDS, p + (t + AHEAD[j]) // KINDS

        @pl.when((q > 0) & (q < pairs))
        def _():
            acts[j](at, q)

    def loop(p, carry):
        for t in range(KINDS):
            send(t, p)
            if t == 0:

                @pl.when(p == 0)
                def _():
                    for j in range(fb + 1):
                        for v in range(KINDS, AHEAD[j]):
                            acts[j](v % KINDS, v // KINDS)

            for j in range(fb, -1, -1):
                later(t, p, j)

        @pl.when(p == 1)
        def _():
            for c in router_copies(1):
                c.wait()
            for c in router_copies(2):
                c.start()

        return carry

    lax.fori_loop(0, pairs, loop, 0)

    for c in router_copies(2):
        c.wait()
    outward = [
        pltpu.make_async_copy(all_ref, all_out, wsem.at[0]),
        pltpu.make_async_copy(scale_ref, scale_out, wsem.at[1]),
    ]
    for c in outward:
        c.start()
    for t in range(KINDS):
        if t in LATE:
            for c in late_copies(t):
                c.wait()
        else:
            finish_bulk(t, last)
        for k in range(1, n):
            arrived = lands[t].at[other(me, k)]
            pltpu.make_async_copy(arrived, arrived, brecv.at[t, k]).wait()
    for c in outward:
        c.wait()


def route(mesh, gate, up, down, weight, gain):
    n_ep, n = mesh.shape["ep"], mesh.shape["fsdp"]
    experts, rows, wide = gate.shape
    piece, fb, pairs = wide // n, bits_of(n), experts // PAIR
    hbm = pl.BlockSpec(memory_space=pl.ANY)
    gathered = jax.ShapeDtypeStruct((n_ep, n // 2, 2) + weight.shape, jnp.bfloat16)
    scales = jax.ShapeDtypeStruct((KINDS, experts, 1, wide), jnp.float32)
    dma = pltpu.SemaphoreType.DMA
    half = jnp.bfloat16
    land = lambda t: jax.ShapeDtypeStruct((n, experts - PAIR * (t in LATE), piece, rows), half)
    outs = pl.pallas_call(
        functools.partial(route_kernel, n_ep, n, pairs),
        out_shape=tuple(land(t) for t in range(KINDS))
        + (scales, gathered)
        + tuple(jax.ShapeDtypeStruct((len(LATE), PAIR, piece, rows), half) for _ in range(n)),
        in_specs=[hbm] * (KINDS + 2),
        out_specs=(hbm,) * (KINDS + 2 + n),
        scratch_shapes=[
            VMEM((SLOTS, PAIR, rows, wide), jnp.float32),
            VMEM((SLOTS, PAIR, rows, wide), jnp.float32),
            VMEM((SLOTS, PAIR, wide, rows), jnp.float32),
            VMEM(weight.shape, weight.dtype),
            VMEM(gain.shape, gain.dtype),
            VMEM(scales.shape, scales.dtype),
            VMEM(gathered.shape, gathered.dtype),
            VMEM((KINDS, n, PAIR, piece, rows), half),
            VMEM((KINDS, SLOTS, PAIR, 1, wide), jnp.float32),
            VMEM((KINDS, SLOTS, fb - 1, 1, wide), jnp.float32),
            VMEM((KINDS, SLOTS, fb, 1, wide), jnp.float32),
            VMEM((KINDS, n, PAIR, 1, wide), jnp.float32),
            dma((KINDS + 2, SLOTS)),
            dma((KINDS, SLOTS, fb + 1)),
            dma((KINDS, SLOTS, fb + 1)),
            dma((KINDS + PAIR - 1, n - 1)),
            dma((KINDS + PAIR - 1, n - 1)),
            dma((KINDS, n)),
            dma((KINDS, n)),
            dma((len(LATE), n)),
            dma((n_ep - 1 + n // 2,)),
            dma((n_ep - 1 + n // 2,)),
            dma((2,)),
        ],
        compiler_params=pltpu.CompilerParams(collective_id=0, has_side_effects=True),
        cost_estimate=pl.CostEstimate(flops=12 * gate.size, bytes_accessed=18 * gate.size, transcendentals=0),
        name="route",
    )(gate, up, down, weight, gain)
    return outs[:KINDS], outs[KINDS], outs[KINDS + 1], outs[KINDS + 2 :]


def place_kernel(counts, *refs):
    lands, outs, (held, isem, osem) = refs[:KINDS], refs[KINDS : 2 * KINDS], refs[2 * KINDS :]
    n, slots = lands[0].shape[0], held.shape[0]
    rows = lands[0].shape[3]
    units = [(t, p) for t in range(KINDS) for p in range(counts[t])]

    def takes(u):
        t, p = units[u]
        return [
            pltpu.make_async_copy(
                lands[t].at[s, pl.ds(p * PAIR, PAIR)],
                held.at[u % slots, :, :, pl.ds(s * rows, rows)],
                isem.at[u % slots, s],
            )
            for s in range(n)
        ]

    def gives(u):
        t, p = units[u]
        return pltpu.make_async_copy(held.at[u % slots], outs[t].at[pl.ds(p * PAIR, PAIR)], osem.at[u % slots])

    behind = slots // 2
    for u in range(len(units) + slots - behind):
        if u < len(units):
            if u >= slots:
                gives(u - slots).wait()
            for c in takes(u):
                c.start()
        v = u - (slots - behind)
        if v >= 0:
            for c in takes(v):
                c.wait()
            gives(v).start()
    for u in range(max(0, len(units) - slots), len(units)):
        gives(u).wait()


def place(lands, experts, slots=8):
    n, _, piece, rows = lands[0].shape
    total = sum(x.size for x in lands)
    out = jax.ShapeDtypeStruct((experts, piece, n * rows), lands[0].dtype)
    hbm = pl.BlockSpec(memory_space=pl.ANY)
    return pl.pallas_call(
        functools.partial(place_kernel, [x.shape[1] // PAIR for x in lands]),
        out_shape=(out,) * KINDS,
        in_specs=[hbm] * KINDS,
        out_specs=(hbm,) * KINDS,
        scratch_shapes=[
            VMEM((slots, PAIR, piece, n * rows), lands[0].dtype),
            pltpu.SemaphoreType.DMA((slots, n)),
            pltpu.SemaphoreType.DMA((slots,)),
        ],
        cost_estimate=pl.CostEstimate(flops=total, bytes_accessed=4 * total, transcendentals=0),
        name="place",
    )(*lands)


def finish_kernel(n, count, *refs):
    got, outs = refs[:n], refs[n + count :]
    me = lax.axis_index("fsdp")
    rows = got[0].shape[3]
    for k in range(n):
        at = pl.multiple_of(other(me, k) * rows, 128)
        for t in range(count):
            outs[t][0, :, pl.ds(at, rows)] = got[k][t, pl.program_id(0)]


def finish(got, arrays):
    n, count = len(got), len(arrays)
    _, _, piece, rows = got[0].shape
    experts = arrays[0].shape[0]
    return pl.pallas_call(
        functools.partial(finish_kernel, n, count),
        grid=(PAIR,),
        out_shape=tuple(jax.ShapeDtypeStruct(a.shape, a.dtype) for a in arrays),
        in_specs=[pl.BlockSpec(memory_space=VMEM)] * n
        + [pl.BlockSpec(memory_space=pl.ANY)] * count,
        out_specs=tuple([pl.BlockSpec((1, piece, n * rows), lambda e: (experts - PAIR + e, 0, 0))] * count),
        input_output_aliases={n + t: t for t in range(count)},
        compiler_params=pltpu.CompilerParams(vmem_limit_bytes=16 << 20),
        cost_estimate=pl.CostEstimate(flops=n * got[0].size, bytes_accessed=4 * n * got[0].size, transcendentals=0),
        name="finish",
    )(*got, *arrays)


def body(mesh, train_gate, train_up, train_down, router_weight, router_gain):
    n = mesh.shape["fsdp"]
    experts, rows, wide = train_gate.shape
    piece = wide // n
    lands, scale, gathered, late = route(
        mesh, train_gate, train_up, train_down, router_weight.T, router_gain[None, :]
    )
    got = [late[0]] * n
    for k in sorted(range(1, n), key=lambda k: (k % 2, k)):
        got[k] = lax.ppermute(late[k], "fsdp", [(i, i ^ k) for i in range(n)])
    placed = list(place(lands, experts))
    done = finish(got, tuple(placed[t] for t in LATE))
    for t, array in zip(LATE, done):
        placed[t] = array
    ready_gate, ready_up, ready_down = placed[0].swapaxes(1, 2), placed[1].swapaxes(1, 2), placed[2]

    mine = lax.dynamic_slice_in_dim(scale[:, :, 0], lax.axis_index("fsdp") * piece, piece, axis=2)
    serve_router = gathered.transpose(0, 3, 1, 2, 4).reshape(-1, n * rows).T
    return (ready_gate, ready_up, ready_down, mine[0], mine[1], mine[2], serve_router)


def solution(mesh):
    def step(gate, up, down, weight, gain):
        n_ep, n = mesh.shape["ep"], mesh.shape["fsdp"]
        experts, rows, wide = gate.shape
        fits = n & (n - 1) == 0 and n_ep > 1 and 2 < n and bits_of(n) + 1 == len(AHEAD)
        if fits and rows % 128 == 0 and wide % (16 * n) == 0 and wide % 128 == 0 and experts % PAIR == 0 and experts >= 8 * PAIR:
            return body(mesh, gate, up, down, weight, gain)
        return plain_body(gate, up, down, weight, gain)

    return jax.shard_map(
        step,
        mesh=mesh,
        in_specs=(
            P("ep", "fsdp", None),
            P("ep", "fsdp", None),
            P("ep", None, "fsdp"),
            P("fsdp", "ep"),
            P("fsdp"),
        ),
        out_specs=(
            P("ep", None, "fsdp"),
            P("ep", None, "fsdp"),
            P("ep", "fsdp", None),
            P("ep", "fsdp"),
            P("ep", "fsdp"),
            P("ep", "fsdp"),
            P(),
        ),
        check_vma=False,
    )
```

```python
import functools

import jax
import jax.numpy as jnp
from jax import lax
from jax.experimental import pallas as pl
from jax.experimental.pallas import tpu as pltpu
from jax.sharding import PartitionSpec as P

MESH = pl.DeviceIdType.MESH
VMEM = pltpu.VMEM
PAIR = 2
SLOTS = 3
KINDS = 3
LATE = (1, 2)
AHEAD = (6, 5, 3, 1)


def bits_of(n):
    return n.bit_length() - 1


def plain_body(train_gate, train_up, train_down, router_weight, router_gain):
    total_gate, total_up, total_down = lax.psum(
        (
            jnp.sum(train_gate * train_gate, axis=1),
            jnp.sum(train_up * train_up, axis=1),
            jnp.sum(train_down * train_down, axis=2),
        ),
        "fsdp",
    )
    scale_gate = jnp.sqrt(total_gate)
    scale_up = jnp.sqrt(total_up)
    scale_down = jnp.sqrt(total_down)
    narrow_gate, narrow_up, narrow_down = (
        (train_gate / jnp.expand_dims(scale_gate, 1)).astype(jnp.bfloat16),
        (train_up / jnp.expand_dims(scale_up, 1)).astype(jnp.bfloat16),
        (train_down / jnp.expand_dims(scale_down, 2)).astype(jnp.bfloat16),
    )
    ready_gate = lax.all_to_all(narrow_gate, "fsdp", split_axis=2, concat_axis=1, tiled=True)
    ready_up = lax.all_to_all(narrow_up, "fsdp", split_axis=2, concat_axis=1, tiled=True)
    ready_down = lax.all_to_all(narrow_down, "fsdp", split_axis=1, concat_axis=2, tiled=True)
    piece = ready_gate.shape[2]
    mine = lambda s: lax.dynamic_slice_in_dim(s, lax.axis_index("fsdp") * piece, piece, axis=1)
    part_router = (router_weight * router_gain[:, None]).astype(jnp.bfloat16)
    row_router = lax.all_gather(part_router, "fsdp", axis=0, tiled=True)
    serve_router = lax.all_gather(row_router, "ep", axis=1, tiled=True)
    return (ready_gate, ready_up, ready_down, mine(scale_gate), mine(scale_up), mine(scale_down), serve_router)


def column_of(row, width):
    return jnp.broadcast_to(row, (width, row.shape[1])).T


def flip(i, w):
    return i + w - 2 * w * ((i // w) % 2)


def other(i, k):
    for b in range(bits_of(k) + 1):
        if (k >> b) & 1:
            i = flip(i, 1 << b)
    return i


def square_sums(turned, x):
    x = x * x
    if turned:
        return jnp.sum(x, axis=0, keepdims=True)
    folded = x[:, :128]
    for at in range(128, x.shape[1], 128):
        folded = folded + x[:, at : at + 128]
    return jnp.sum(folded.T, axis=0, keepdims=True)


def route_kernel(n_ep, n, pairs, *refs):
    fb = bits_of(n)
    sources, (weight_src, gain_src), refs = refs[:KINDS], refs[KINDS : KINDS + 2], refs[KINDS + 2 :]
    lands, (scale_out, all_out), refs = refs[:KINDS], refs[KINDS : KINDS + 2], refs[KINDS + 2 :]
    late_refs, refs = refs[:n], refs[n:]
    held, refs = refs[:KINDS], refs[KINDS:]
    weight_ref, gain_ref, scale_ref, all_ref, packed, part, total, landed, first = refs[:9]
    lsem, ssend, srecv, fsend, frecv, bsend, brecv, osem, rsend, rrecv, wsem = refs[9:]
    ep, me = lax.axis_index("ep"), lax.axis_index("fsdp")
    core = me % 2
    piece = packed.shape[3]
    last = pairs - 1

    ep_peers = [((ep + d) % n_ep, me) for d in range(1, n_ep)]
    fsdp_peers = [(ep, other(me, k)) for k in range(1, n)]
    sum_peers = [(ep, flip(me, 1))] + [
        (ep, flip(me, (1 << k) * (1 - core) + (1 << (fb - k)) * core)) for k in range(1, fb)
    ]

    def load(t, p):
        return pltpu.make_async_copy(
            sources[t].at[pl.ds(p * PAIR, PAIR)], held[t].at[p % SLOTS], lsem.at[t, p % SLOTS]
        )

    opening = [(0, i, 1) for i in range(PAIR)] + [(t, 0, PAIR) for t in range(1, KINDS)]

    def first_load(at):
        t, i, count = opening[at]
        return pltpu.make_async_copy(
            sources[t].at[pl.ds(i, count)], held[t].at[0, pl.ds(i, count)], lsem.at[KINDS + at // SLOTS, at % SLOTS]
        )

    def first_copies(at):
        t, i, count = opening[at]
        return [
            pltpu.make_async_remote_copy(
                part.at[t, 0, pl.ds(i, count)],
                first.at[t, me, pl.ds(i, count)],
                fsend.at[at, k - 1],
                frecv.at[at, k - 1],
                device_id=fsdp_peers[k - 1],
                device_id_type=MESH,
            )
            for k in range(1, n)
        ]

    def first_scales(at):
        t, i, count = opening[at]
        for c in first_copies(at):
            c.wait()
        rows = pl.ds(i, count)
        first[t, me, rows] = part[t, 0, rows]
        value = first[t, 0, rows]
        for j in range(1, n):
            value = value + first[t, j, rows]
        scale_ref[t, rows] = jnp.sqrt(value)

    weight_loads = [
        pltpu.make_async_copy(weight_src, weight_ref, wsem.at[0]),
        pltpu.make_async_copy(gain_src, gain_ref, wsem.at[1]),
    ]
    first_load(0).start()
    for c in weight_loads:
        c.start()
    first_load(1).start()
    barrier = pltpu.get_barrier_semaphore()
    for peer in ep_peers + fsdp_peers:
        pl.semaphore_signal(barrier, inc=1, device_id=peer, device_id_type=MESH)

    def sum_copy(k, t, p):
        s = p % SLOTS
        if k == 0:
            src, dst, peer = part.at[t, s, 1 - core], landed.at[t, s, 0], sum_peers[0]
        elif k < fb:
            src, dst, peer = total.at[t, s, k - 1], landed.at[t, s, k], sum_peers[k]
        else:
            src = dst = scale_ref.at[t, p * PAIR + core]
            peer = sum_peers[0]
        return pltpu.make_async_remote_copy(
            src, dst, ssend.at[t, s, k], srecv.at[t, s, k], device_id=peer, device_id_type=MESH
        )

    def begin_sums(t, p):
        s = p % SLOTS
        load(t, p).wait()
        for i in range(PAIR):
            part[t, s, i] = square_sums(t < 2, held[t][s, i])
        sum_copy(0, t, p).start()

    def step_sums(k, t, p):
        s = p % SLOTS
        sum_copy(k, t, p).wait()
        value = (part[t, s, core] if k == 0 else total[t, s, k - 1]) + landed[t, s, k]
        if k < fb - 1:
            total[t, s, k] = value
        else:
            scale_ref[t, p * PAIR + core] = jnp.sqrt(value)
        sum_copy(k + 1, t, p).start()

    nearest = sorted(range(1, n), key=lambda k: (k < 2, bin(k // 2).count("1"), k % 2, -k))

    def bulk_copies(t, p, i, count):
        dst = lands[t].at[me, pl.ds(p * PAIR + i, count)]
        copies = [
            pltpu.make_async_remote_copy(
                packed.at[t, other(me, k), pl.ds(i, count)],
                dst,
                bsend.at[t, k],
                brecv.at[t, k],
                device_id=(ep, other(me, k)),
                device_id_type=MESH,
            )
            for k in nearest
        ]
        return copies, pltpu.make_async_copy(packed.at[t, me, pl.ds(i, count)], dst, bsend.at[t, 0])

    def start_bulk(t, p, i, count):
        remote, local = bulk_copies(t, p, i, count)
        for c in remote:
            c.start()
        local.start()

    def finish_bulk(t, p):
        remote, local = bulk_copies(t, p, 0, PAIR)
        for c in remote:
            c.wait_send()
        local.wait()

    def late_copies(t):
        at = LATE.index(t)
        return [
            pltpu.make_async_copy(packed.at[t, other(me, k)], late_refs[k].at[at], osem.at[at, k]) for k in range(n)
        ]

    def send(t, p):
        s = p % SLOTS

        @pl.when(p > 0)
        def _():
            sum_copy(fb, t, p).wait()
            finish_bulk(t, p - 1)

        for i in range(PAIR):

            @pl.when(p == 0)
            def _():
                if (t, i, 1) in opening:
                    first_scales(opening.index((t, i, 1)))
                elif i == 0:
                    first_scales(opening.index((t, i, PAIR)))

            inverse = 1.0 / scale_ref[t, p * PAIR + i]
            if t < 2:
                y = (held[t][s, i] * inverse).astype(packed.dtype).T
                for j in range(n):
                    packed[t, j, i] = y[j * piece : (j + 1) * piece, :]
            else:
                column = column_of(inverse, 128)
                for at in range(0, held[t].shape[3], 128):
                    y = (held[t][s, i, :, at : at + 128] * column).astype(packed.dtype)
                    for j in range(n):
                        packed[t, j, i, :, at : at + 128] = y[j * piece : (j + 1) * piece, :]
            if (t, i, 1) in opening:

                @pl.when(p == 0)
                def _():
                    start_bulk(t, p, i, 1)

        split = (t, 0, 1) in opening

        @pl.when((p >= split) & (p < last + (t not in LATE)))
        def _():
            start_bulk(t, p, 0, PAIR)

        if t in LATE:

            @pl.when(p == last)
            def _():
                for c in late_copies(t):
                    c.start()

        @pl.when(p + SLOTS < pairs)
        def _():
            load(t, p + SLOTS).start()

    def router_copies(k):
        if k == 0:
            block = all_ref.at[ep, me // 2, core]
            jobs = [(c - 1, fsdp_peers[2 * c - 1]) for c in range(1, n // 2)]
        elif k == 1:
            block = all_ref.at[ep, :, core]
            jobs = [(n // 2 - 1, sum_peers[0])]
        else:
            block = all_ref.at[ep]
            jobs = [(n // 2 + d, peer) for d, peer in enumerate(ep_peers)]
        return [
            pltpu.make_async_remote_copy(block, block, rsend.at[i], rrecv.at[i], device_id=peer, device_id_type=MESH)
            for i, peer in jobs
        ]

    for at, (t, i, count) in enumerate(opening):
        first_load(at).wait()
        if at + 2 < len(opening):
            first_load(at + 2).start()
        for e in range(i, i + count):
            part[t, 0, e] = square_sums(t < 2, held[t][0, e])
        if at == 0:
            pl.semaphore_wait(barrier, n_ep - 1 + n - 1)
        for c in first_copies(at):
            c.start()
        if at == 0:
            for c in weight_loads:
                c.wait()
            all_ref[ep, me // 2, core] = (weight_ref[...] * gain_ref[...]).astype(all_ref.dtype)
            for c in router_copies(0):
                c.start()
    for p in range(1, SLOTS):
        for t in range(KINDS):
            load(t, p).start()

    acts = [begin_sums] + [functools.partial(step_sums, k) for k in range(fb)]

    def later(t, p, j):
        at, q = (t + AHEAD[j]) % KINDS, p + (t + AHEAD[j]) // KINDS

        @pl.when((q > 0) & (q < pairs))
        def _():
            acts[j](at, q)

    def loop(p, carry):
        for t in range(KINDS):
            send(t, p)
            if t == 0:

                @pl.when(p == 0)
                def _():
                    for j in range(fb + 1):
                        for v in range(KINDS, AHEAD[j]):
                            acts[j](v % KINDS, v // KINDS)

            for j in range(fb, -1, -1):
                later(t, p, j)

        for k in (1, 2):

            @pl.when(p == k - 1)
            def _():
                for c in router_copies(k - 1):
                    c.wait()
                for c in router_copies(k):
                    c.start()

        return carry

    lax.fori_loop(0, pairs, loop, 0)

    for c in router_copies(2):
        c.wait()
    outward = [
        pltpu.make_async_copy(all_ref, all_out, wsem.at[0]),
        pltpu.make_async_copy(scale_ref, scale_out, wsem.at[1]),
    ]
    for c in outward:
        c.start()
    for t in range(KINDS):
        if t in LATE:
            for c in late_copies(t):
                c.wait()
        else:
            finish_bulk(t, last)
        for k in range(1, n):
            arrived = lands[t].at[other(me, k)]
            pltpu.make_async_copy(arrived, arrived, brecv.at[t, k]).wait()
    for c in outward:
        c.wait()


def route(mesh, gate, up, down, weight, gain):
    n_ep, n = mesh.shape["ep"], mesh.shape["fsdp"]
    experts, rows, wide = gate.shape
    piece, fb, pairs = wide // n, bits_of(n), experts // PAIR
    hbm = pl.BlockSpec(memory_space=pl.ANY)
    gathered = jax.ShapeDtypeStruct((n_ep, n // 2, 2) + weight.shape, jnp.bfloat16)
    scales = jax.ShapeDtypeStruct((KINDS, experts, 1, wide), jnp.float32)
    dma = pltpu.SemaphoreType.DMA
    half = jnp.bfloat16
    land = lambda t: jax.ShapeDtypeStruct((n, experts - PAIR * (t in LATE), piece, rows), half)
    outs = pl.pallas_call(
        functools.partial(route_kernel, n_ep, n, pairs),
        out_shape=tuple(land(t) for t in range(KINDS))
        + (scales, gathered)
        + tuple(jax.ShapeDtypeStruct((len(LATE), PAIR, piece, rows), half) for _ in range(n)),
        in_specs=[hbm] * (KINDS + 2),
        out_specs=(hbm,) * (KINDS + 2 + n),
        scratch_shapes=[
            VMEM((SLOTS, PAIR, rows, wide), jnp.float32),
            VMEM((SLOTS, PAIR, rows, wide), jnp.float32),
            VMEM((SLOTS, PAIR, wide, rows), jnp.float32),
            VMEM(weight.shape, weight.dtype),
            VMEM(gain.shape, gain.dtype),
            VMEM(scales.shape, scales.dtype),
            VMEM(gathered.shape, gathered.dtype),
            VMEM((KINDS, n, PAIR, piece, rows), half),
            VMEM((KINDS, SLOTS, PAIR, 1, wide), jnp.float32),
            VMEM((KINDS, SLOTS, fb - 1, 1, wide), jnp.float32),
            VMEM((KINDS, SLOTS, fb, 1, wide), jnp.float32),
            VMEM((KINDS, n, PAIR, 1, wide), jnp.float32),
            dma((KINDS + 2, SLOTS)),
            dma((KINDS, SLOTS, fb + 1)),
            dma((KINDS, SLOTS, fb + 1)),
            dma((KINDS + PAIR - 1, n - 1)),
            dma((KINDS + PAIR - 1, n - 1)),
            dma((KINDS, n)),
            dma((KINDS, n)),
            dma((len(LATE), n)),
            dma((n_ep - 1 + n // 2,)),
            dma((n_ep - 1 + n // 2,)),
            dma((2,)),
        ],
        compiler_params=pltpu.CompilerParams(collective_id=0, has_side_effects=True),
        cost_estimate=pl.CostEstimate(flops=12 * gate.size, bytes_accessed=18 * gate.size, transcendentals=0),
        name="route",
    )(gate, up, down, weight, gain)
    return outs[:KINDS], outs[KINDS], outs[KINDS + 1], outs[KINDS + 2 :]


def place_kernel(counts, *refs):
    lands, outs, (held, isem, osem) = refs[:KINDS], refs[KINDS : 2 * KINDS], refs[2 * KINDS :]
    n, slots = lands[0].shape[0], held.shape[0]
    rows = lands[0].shape[3]
    units = [(t, p) for t in range(KINDS) for p in range(counts[t])]

    def takes(u):
        t, p = units[u]
        return [
            pltpu.make_async_copy(
                lands[t].at[s, pl.ds(p * PAIR, PAIR)],
                held.at[u % slots, :, :, pl.ds(s * rows, rows)],
                isem.at[u % slots, s],
            )
            for s in range(n)
        ]

    def gives(u):
        t, p = units[u]
        return pltpu.make_async_copy(held.at[u % slots], outs[t].at[pl.ds(p * PAIR, PAIR)], osem.at[u % slots])

    behind = slots // 2
    for u in range(len(units) + slots - behind):
        if u < len(units):
            if u >= slots:
                gives(u - slots).wait()
            for c in takes(u):
                c.start()
        v = u - (slots - behind)
        if v >= 0:
            for c in takes(v):
                c.wait()
            gives(v).start()
    for u in range(max(0, len(units) - slots), len(units)):
        gives(u).wait()


def place(lands, experts, slots=8):
    n, _, piece, rows = lands[0].shape
    total = sum(x.size for x in lands)
    out = jax.ShapeDtypeStruct((experts, piece, n * rows), lands[0].dtype)
    hbm = pl.BlockSpec(memory_space=pl.ANY)
    return pl.pallas_call(
        functools.partial(place_kernel, [x.shape[1] // PAIR for x in lands]),
        out_shape=(out,) * KINDS,
        in_specs=[hbm] * KINDS,
        out_specs=(hbm,) * KINDS,
        scratch_shapes=[
            VMEM((slots, PAIR, piece, n * rows), lands[0].dtype),
            pltpu.SemaphoreType.DMA((slots, n)),
            pltpu.SemaphoreType.DMA((slots,)),
        ],
        cost_estimate=pl.CostEstimate(flops=total, bytes_accessed=4 * total, transcendentals=0),
        name="place",
    )(*lands)


def finish_kernel(n, count, *refs):
    got, outs = refs[:n], refs[n + count :]
    me = lax.axis_index("fsdp")
    rows = got[0].shape[3]
    for k in range(n):
        at = pl.multiple_of(other(me, k) * rows, 128)
        for t in range(count):
            outs[t][0, :, pl.ds(at, rows)] = got[k][t, pl.program_id(0)]


def finish(got, arrays):
    n, count = len(got), len(arrays)
    _, _, piece, rows = got[0].shape
    experts = arrays[0].shape[0]
    return pl.pallas_call(
        functools.partial(finish_kernel, n, count),
        grid=(PAIR,),
        out_shape=tuple(jax.ShapeDtypeStruct(a.shape, a.dtype) for a in arrays),
        in_specs=[pl.BlockSpec(memory_space=VMEM)] * n
        + [pl.BlockSpec(memory_space=pl.ANY)] * count,
        out_specs=tuple([pl.BlockSpec((1, piece, n * rows), lambda e: (experts - PAIR + e, 0, 0))] * count),
        input_output_aliases={n + t: t for t in range(count)},
        compiler_params=pltpu.CompilerParams(vmem_limit_bytes=16 << 20),
        cost_estimate=pl.CostEstimate(flops=n * got[0].size, bytes_accessed=4 * n * got[0].size, transcendentals=0),
        name="finish",
    )(*got, *arrays)


def body(mesh, train_gate, train_up, train_down, router_weight, router_gain):
    n = mesh.shape["fsdp"]
    experts, rows, wide = train_gate.shape
    piece = wide // n
    lands, scale, gathered, late = route(
        mesh, train_gate, train_up, train_down, router_weight.T, router_gain[None, :]
    )
    got = [late[0]] * n
    for k in sorted(range(1, n), key=lambda k: (k % 2, k)):
        got[k] = lax.ppermute(late[k], "fsdp", [(i, i ^ k) for i in range(n)])
    placed = list(place(lands, experts))
    done = finish(got, tuple(placed[t] for t in LATE))
    for t, array in zip(LATE, done):
        placed[t] = array
    ready_gate, ready_up, ready_down = placed[0].swapaxes(1, 2), placed[1].swapaxes(1, 2), placed[2]

    mine = lax.dynamic_slice_in_dim(scale[:, :, 0], lax.axis_index("fsdp") * piece, piece, axis=2)
    serve_router = gathered.transpose(0, 3, 1, 2, 4).reshape(-1, n * rows).T
    return (ready_gate, ready_up, ready_down, mine[0], mine[1], mine[2], serve_router)


def solution(mesh):
    def step(gate, up, down, weight, gain):
        n_ep, n = mesh.shape["ep"], mesh.shape["fsdp"]
        experts, rows, wide = gate.shape
        fits = n & (n - 1) == 0 and n_ep > 1 and 2 < n and bits_of(n) + 1 == len(AHEAD)
        if fits and rows % 128 == 0 and wide % (16 * n) == 0 and wide % 128 == 0 and experts % PAIR == 0 and experts >= 8 * PAIR:
            return body(mesh, gate, up, down, weight, gain)
        return plain_body(gate, up, down, weight, gain)

    return jax.shard_map(
        step,
        mesh=mesh,
        in_specs=(
            P("ep", "fsdp", None),
            P("ep", "fsdp", None),
            P("ep", None, "fsdp"),
            P("fsdp", "ep"),
            P("fsdp"),
        ),
        out_specs=(
            P("ep", None, "fsdp"),
            P("ep", None, "fsdp"),
            P("ep", "fsdp", None),
            P("ep", "fsdp"),
            P("ep", "fsdp"),
            P("ep", "fsdp"),
            P(),
        ),
        check_vma=False,
    )
```
